32 devices in a mesh: dp: 4 (over x, core), mp: 8 (over z, y).
Axes of the slice: x: 2, y: 2, z: 4, core: 2. Of those that a mesh axis runs over, the one named last changes fastest.
Arguments:
- tokens: bfloat16 [128, 8192], P('dp', 'mp'), may hold values from -6 to 6
- gate_up_weight: bfloat16 [2, 8192, 15360], P(None, 'mp', 'dp'), may hold values from -0.0625 to 0.0625
- down_weight: bfloat16 [15360, 8192], P('dp', 'mp'), may hold values from -0.046875 to 0.046875
- gate_up_input_factor: bfloat16 [2, 8192, 64], P(None, 'mp'), may hold values from -0.0625 to 0.0625
- gate_up_output_factor: bfloat16 [2, 64, 15360], P(None, None, 'dp'), may hold values from -0.046875 to 0.046875
- down_input_factor: bfloat16 [15360, 64], P('dp'), may hold values from -0.046875 to 0.046875
- down_output_factor: bfloat16 [64, 8192], P(None, 'mp'), may hold values from -0.0625 to 0.0625
- cotangent: bfloat16 [128, 8192], P('dp', 'mp'), may hold values from -6 to 6
Outputs:
- output: bfloat16 [128, 8192], P('dp', 'mp')
- input_grad: bfloat16 [128, 8192], P('dp', 'mp')
- grad_gate_up_lower: float32 [2, 8192, 64], P(None, 'mp')
- gate_up_output_factor_gradient: float32 [2, 64, 15360], P(None, None, 'dp')
- down_input_factor_gradient: float32 [15360, 64], P('dp')
- down_output_factor_gradient: float32 [64, 8192], P(None, 'mp')
The draws below stay inside these ranges and needn't reach their ends.
All inputs are finite; a program needn't handle non-finite values.
Results may differ from the reference program's by a relative error of at most 0.0065.
Values may be sent and summed in bfloat16 or wider, within the bound.
A program may use at most 64 MiB of HBM per device.

```python
import jax
import jax.numpy as jnp
from jax import lax

D = 8192
FF = 15360
R = 64
TOKENS = 128


def steps_of(key, dims, cuts, low, high):
    loudness = 1.0
    for dim, parts in cuts:
        draws = jax.random.uniform(jax.random.fold_in(jax.random.fold_in(key, 6), dim), (parts,), jnp.float32, low / len(cuts), high / len(cuts))
        loudness = loudness * jnp.repeat(jnp.exp(draws), dims[dim] // parts).reshape((-1,) + (1,) * (len(dims) - 1 - dim))
    return loudness


def normal_values(stream_key, shape, width, bound, split=(), dtype=jnp.bfloat16):
    gain = steps_of(stream_key, shape, split, -0.22, 0.18) if split else 1.0
    values = jax.random.normal(stream_key, shape, jnp.float32) * width * gain
    return jnp.minimum(jnp.maximum(values, -bound), bound).astype(dtype)


def setup_inputs(seed: int = 0) -> dict:
    key_of = jax.random.split(jax.random.key(seed), 9)
    tokens = normal_values(key_of[0], (TOKENS, D), 1.0, 6.0, ((0, 4), (1, 8)))
    gate_up_weight = normal_values(key_of[1], (2, D, FF), D ** -0.5, 0.0625, ((1, 8), (2, 4)))
    down_weight = normal_values(key_of[2], (FF, D), FF ** -0.5, 0.046875, ((0, 4), (1, 8)))
    gate_up_input_factor = normal_values(key_of[3], (2, D, R), D ** -0.5, 0.0625, ((1, 8),))
    gate_up_output_factor = normal_values(key_of[4], (2, R, FF), FF ** -0.5, 0.046875, ((2, 4),))
    down_input_factor = normal_values(key_of[5], (FF, R), FF ** -0.5, 0.046875, ((0, 4),))
    down_output_factor = normal_values(key_of[6], (R, D), D ** -0.5, 0.0625, ((1, 8),))
    cotangent = normal_values(key_of[7], (TOKENS, D), 1.0, 6.0, ((0, 4), (1, 8)))
    return {"tokens": tokens, "gate_up_weight": gate_up_weight, "down_weight": down_weight, "gate_up_input_factor": gate_up_input_factor, "gate_up_output_factor": gate_up_output_factor, "down_input_factor": down_input_factor, "down_output_factor": down_output_factor, "cotangent": cotangent}


adapter_scale = 2.0


def reference(tokens, gate_up_weight, down_weight, gate_up_input_factor, gate_up_output_factor, down_input_factor, down_output_factor, cotangent):
    single_float = jnp.float32
    upper_projection = lax.Precision.HIGHEST
    scale_factor = TOKENS ** -0.5
    lower_results = []
    pres = []
    for rank_dimension in range(2):
        lower_projection = jnp.dot(tokens, gate_up_input_factor[rank_dimension], preferred_element_type=single_float)
        lower_results.append(lower_projection)
        preactivation = jnp.dot(tokens, gate_up_weight[rank_dimension], preferred_element_type=single_float)
        preactivation = preactivation + adapter_scale * jnp.dot(lower_projection, gate_up_output_factor[rank_dimension].astype(single_float), precision=upper_projection)
        pres.append(preactivation)
    gate, upper = pres[0], pres[1]
    hidden_state = (jax.nn.silu(gate) * upper).astype(jnp.bfloat16)
    lower_down_projection = jnp.dot(hidden_state, down_input_factor, preferred_element_type=single_float)
    output = jnp.dot(hidden_state, down_weight, preferred_element_type=single_float)
    output = output + adapter_scale * jnp.dot(lower_down_projection, down_output_factor.astype(single_float), precision=upper_projection)
    output = output.astype(jnp.bfloat16)
    backward_down_rows = jnp.dot(cotangent, down_output_factor.T, preferred_element_type=single_float).astype(jnp.bfloat16)
    hidden_state_gradient = jnp.dot(cotangent, down_weight.T, preferred_element_type=single_float)
    hidden_state_gradient = hidden_state_gradient + adapter_scale * jnp.dot(backward_down_rows, down_input_factor.T, preferred_element_type=single_float)
    down_input_factor_gradient = adapter_scale * scale_factor * jnp.dot(hidden_state.T, backward_down_rows, preferred_element_type=single_float)
    down_output_factor_gradient = adapter_scale * scale_factor * jnp.dot(lower_down_projection.T, cotangent.astype(single_float), precision=upper_projection)
    sigma = jax.nn.sigmoid(gate)
    gate_back = (hidden_state_gradient * upper * sigma * (1.0 + gate * (1.0 - sigma))).astype(jnp.bfloat16)
    up_back = (hidden_state_gradient * gate * sigma).astype(jnp.bfloat16)
    backward_results = [gate_back, up_back]
    output_factor_gradient = []
    input_factor_gradient = []
    input_total_sum = jnp.zeros(tokens.shape, single_float)
    for rank_dimension in range(2):
        output_factor_gradient.append(adapter_scale * scale_factor * jnp.dot(lower_results[rank_dimension].T, backward_results[rank_dimension].astype(single_float), precision=upper_projection))
        backward_lower_rows = jnp.dot(backward_results[rank_dimension], gate_up_output_factor[rank_dimension].T, preferred_element_type=single_float).astype(jnp.bfloat16)
        input_factor_gradient.append(adapter_scale * scale_factor * jnp.dot(tokens.T, backward_lower_rows, preferred_element_type=single_float))
        input_total_sum = input_total_sum + jnp.dot(backward_results[rank_dimension], gate_up_weight[rank_dimension].T, preferred_element_type=single_float)
        input_total_sum = input_total_sum + adapter_scale * jnp.dot(backward_lower_rows, gate_up_input_factor[rank_dimension].T, preferred_element_type=single_float)
    input_grad = input_total_sum.astype(jnp.bfloat16)
    return (output, input_grad, jnp.stack(input_factor_gradient), jnp.stack(output_factor_gradient), down_input_factor_gradient, down_output_factor_gradient)
```

```python
import jax
import jax.numpy as jnp
from jax import lax
from jax.experimental import pallas as pl
from jax.experimental.pallas import tpu as pltpu
from jax.sharding import PartitionSpec as P

adapter_scale = 2.0
MESH = pl.DeviceIdType.MESH
F32 = jnp.float32
BF16 = jnp.bfloat16
HIGHEST = lax.Precision.HIGHEST


def dot(left, right, left_dim, right_dim, precision=None):
    return lax.dot_general(
        left,
        right,
        (((left_dim,), (right_dim,)), ((), ())),
        preferred_element_type=F32,
        precision=precision,
    )


def greet(axis, peers):
    barrier = pltpu.get_barrier_semaphore()
    for peer in peers:
        pl.semaphore_signal(barrier, inc=1, device_id={axis: peer}, device_id_type=MESH)
    pl.semaphore_wait(barrier, len(peers))


def remote(axis, peer, source, target, send_sem, recv_sem):
    copy = pltpu.make_async_remote_copy(
        src_ref=source,
        dst_ref=target,
        send_sem=send_sem,
        recv_sem=recv_sem,
        device_id={axis: peer},
        device_id_type=MESH,
    )
    copy.start()
    return copy


def gather_kernel(n, tok_ref, cot_ref, tok_out, cot_out, send_sem, recv_sem):
    me = lax.axis_index("dp")
    rows = tok_ref.shape[0]
    mine = pl.ds(pl.multiple_of(me * rows, rows), rows)
    peers = [lax.rem(me + o, n) for o in range(1, n)]
    greet("dp", peers)
    copies = []
    for a, (source, target) in enumerate(((tok_ref, tok_out), (cot_ref, cot_out))):
        for o, peer in enumerate(peers):
            copies.append(
                remote("dp", peer, source, target.at[mine], send_sem.at[a, o], recv_sem.at[a, o])
            )
    tok_out[mine, :] = tok_ref[...]
    cot_out[mine, :] = cot_ref[...]
    for copy in copies:
        copy.wait()


def middle_kernel(
    n_outer,
    n_inner,
    rows,
    rank,
    small_ref,
    pre_ref,
    back_ref,
    upper_ref,
    down_ref,
    small_out,
    hidden_out,
    grad_out,
    small_in,
    pre_in,
    back_in,
    small_sum,
    pre_sum,
    back_sum,
    small_far,
    pre_far,
    back_far,
    inner_send,
    inner_recv,
    outer_send,
    outer_recv,
    gather_send,
    gather_recv,
    spread_send,
    spread_recv,
):
    me = lax.axis_index("mp")
    outer = me // n_inner
    inner = lax.rem(me, n_inner)

    def place(o, i):
        return lax.rem(outer + o, n_outer) * n_inner + lax.rem(inner + i, n_inner)

    def block(index):
        return pl.ds(pl.multiple_of(index * rows, rows), rows)

    peers = [place(0, i) for i in range(1, n_inner)] + [place(o, 0) for o in range(1, n_outer)]
    greet("mp", peers)

    order = sorted(range(1, n_outer), key=lambda o: -min(o, n_outer - o)) + [0]
    groups = (
        (small_ref, small_in, small_sum, small_far),
        (pre_ref, pre_in, pre_sum, pre_far),
        (back_ref, back_in, back_sum, back_far),
    )

    def part(ref, index):
        return ref.at[:, block(index), :]

    near = {}
    for a, (source, landing, _, _) in enumerate(groups):
        for o in order:
            for i in range(1, n_inner):
                near[a, o, i] = remote(
                    "mp",
                    place(0, i),
                    part(source, place(o, i)),
                    landing.at[i - 1, o],
                    inner_send.at[a, i - 1, o],
                    inner_recv.at[a, i - 1, o],
                )
    far = {}

    def near_total(a, o):
        source, landing, _, _ = groups[a]
        total = source[:, block(place(o, 0)), :].astype(F32)
        for i in range(1, n_inner):
            near[a, o, i].wait_recv()
            total = total + landing[i - 1, o].astype(F32)
        return total

    for a in range(3):
        for o in order[:-1]:
            groups[a][2][o - 1] = near_total(a, o).astype(BF16)
            far[a, o] = remote(
                "mp",
                place(o, 0),
                groups[a][2].at[o - 1],
                groups[a][3].at[o - 1],
                outer_send.at[a, o - 1],
                outer_recv.at[a, o - 1],
            )

    def full_total(a):
        total = near_total(a, 0)
        for o in order[:-1]:
            far[a, o].wait_recv()
            total = total + groups[a][3][o - 1].astype(F32)
        return total

    sent = []
    arrived = {}
    outs = (small_out, hidden_out, grad_out)

    def give(a):
        source = part(outs[a], me)
        for o in order[:-1]:
            arrived[a, o] = remote(
                "mp", place(o, 0), source, source, gather_send.at[a, o - 1], gather_recv.at[a, o - 1]
            )
            sent.append(arrived[a, o])
        spread(a, 0, source)

    def spread(a, o, source):
        for i in range(1, n_inner):
            copy = remote(
                "mp",
                place(0, i),
                source,
                source,
                spread_send.at[a, i - 1, o],
                spread_recv.at[a, i - 1, o],
            )
            sent.append(copy)
            spreads.append(copy)

    spreads = []
    small = full_total(0)[0]
    small_out[0, block(me), :] = small.astype(BF16)
    give(0)
    pre = full_total(1)
    gate = pre[0] + adapter_scale * dot(
        small[:, :rank], upper_ref[0].astype(F32), 1, 0, HIGHEST
    )
    upper = pre[1] + adapter_scale * dot(
        small[:, rank : 2 * rank], upper_ref[1].astype(F32), 1, 0, HIGHEST
    )
    sigma = 1.0 / (1.0 + jnp.exp(-gate))
    hidden_out[0, block(me), :] = (gate * sigma * upper).astype(BF16)
    give(1)
    back_down = small[:, 2 * rank : 3 * rank].astype(BF16)
    hidden_back = full_total(2)[0] + adapter_scale * dot(back_down, down_ref[...], 1, 1)
    grad_out[0, block(me), :] = (
        hidden_back * upper * sigma * (1.0 + gate * (1.0 - sigma))
    ).astype(BF16)
    grad_out[1, block(me), :] = (hidden_back * gate * sigma).astype(BF16)
    give(2)
    for a in range(3):
        for o in order[:-1]:
            arrived[a, o].wait_recv()
            spread(a, o, part(outs[a], place(n_outer - o, 0)))
    for copy in spreads:
        copy.wait_recv()
    for copy in list(near.values()) + list(far.values()) + sent:
        copy.wait_send()


def final_kernel(
    n, rows, out_ref, in_ref, small_ref, out_sum, in_sum, small_sum, out_far, in_far, small_far, send_sem, recv_sem
):
    me = lax.axis_index("dp")

    def block(index):
        return pl.ds(pl.multiple_of(index * rows, rows), rows)

    peers = [lax.rem(me + o, n) for o in range(1, n)]
    greet("dp", peers)
    copies = []
    for o, peer in enumerate(peers):
        copies.append(
            remote("dp", peer, small_ref, small_far.at[o], send_sem.at[0, o], recv_sem.at[0, o])
        )
    for a, (source, landing) in enumerate(((out_ref, out_far), (in_ref, in_far))):
        for o, peer in enumerate(peers):
            copies.append(
                remote(
                    "dp",
                    peer,
                    source.at[block(peer)],
                    landing.at[o],
                    send_sem.at[a + 1, o],
                    recv_sem.at[a + 1, o],
                )
            )
    for copy in copies:
        copy.wait()
    small = small_ref[...].astype(F32)
    total_out = out_ref[block(me), :].astype(F32)
    total_in = in_ref[block(me), :].astype(F32)
    for o in range(n - 1):
        small = small + small_far[o].astype(F32)
        total_out = total_out + out_far[o].astype(F32)
        total_in = total_in + in_far[o].astype(F32)
    small_sum[...] = small
    out_sum[...] = total_out
    in_sum[...] = total_in


def vmem(count):
    return [pl.BlockSpec(memory_space=pltpu.VMEM)] * count


def shape(dims, dtype):
    return jax.ShapeDtypeStruct(dims, dtype)


def communicate(kernel, name, outs, scratch, collective_id, args):
    return pl.pallas_call(
        kernel,
        name=name,
        out_shape=outs,
        in_specs=vmem(len(args)),
        out_specs=vmem(len(outs)),
        scratch_shapes=scratch,
        compiler_params=pltpu.CompilerParams(
            collective_id=collective_id, has_side_effects=True, vmem_limit_bytes=48 * 1024 * 1024
        ),
    )(*args)


def inner_size(n):
    size = 1
    while size * size * 4 <= n:
        size *= 2
    return size


def pad(array):
    width = array.shape[-1]
    extra = -width % 128
    return jnp.pad(array, ((0, 0), (0, extra))) if extra else array


def per_device(
    tokens,
    gate_up_weight,
    down_weight,
    gate_up_input_factor,
    gate_up_output_factor,
    down_input_factor,
    down_output_factor,
    cotangent,
):
    n_dp, n_mp = lax.axis_size("dp"), lax.axis_size("mp")
    tok_rows, width = tokens.shape
    rank, hidden = gate_up_output_factor.shape[1:]
    total = tok_rows * n_dp
    mp_rows = total // n_mp
    gradient_scale = adapter_scale * total ** (-0.5)
    dma = pltpu.SemaphoreType.DMA

    tok, cot = communicate(
        lambda *refs: gather_kernel(n_dp, *refs),
        "gather_rows",
        [shape((total, width), BF16)] * 2,
        [dma((2, n_dp - 1))] * 2,
        0,
        (tokens, cotangent),
    )

    low = jnp.einsum("td,kdr->tkr", tok, gate_up_input_factor, preferred_element_type=F32)
    back_down_part = dot(cot, down_output_factor, 1, 1)
    small = pad(jnp.concatenate([low.reshape(total, 2 * rank), back_down_part], axis=1)).astype(BF16)
    pre = jnp.einsum("td,kdf->ktf", tok, gate_up_weight, preferred_element_type=F32).astype(BF16)
    back = dot(cot, down_weight, 1, 1).astype(BF16)

    n_inner = inner_size(n_mp)
    n_outer = n_mp // n_inner
    small_width = small.shape[1]
    leads, widths = (1, 2, 1), (small_width, hidden, hidden)

    def slots(*count):
        return [pltpu.VMEM((*count, k, mp_rows, w), BF16) for k, w in zip(leads, widths)]

    small_all, hidden_all, grad_all = communicate(
        lambda *refs: middle_kernel(n_outer, n_inner, mp_rows, rank, *refs),
        "middle",
        [
            shape((1, total, small_width), BF16),
            shape((1, total, hidden), BF16),
            shape((2, total, hidden), BF16),
        ],
        [
            *slots(n_inner - 1, n_outer),
            *slots(n_outer - 1),
            *slots(n_outer - 1),
            *[dma((3, n_inner - 1, n_outer))] * 2,
            *[dma((3, n_outer - 1))] * 2,
            *[dma((3, n_outer - 1))] * 2,
            *[dma((3, n_inner - 1, n_outer))] * 2,
        ],
        1,
        (small[None], pre, back[None], gate_up_output_factor, down_input_factor),
    )
    small_all, hidden_all = small_all[0], hidden_all[0]
    back_down = small_all[:, 2 * rank : 3 * rank]

    out_part = dot(hidden_all, down_weight, 1, 0).astype(BF16)
    in_part = jnp.einsum(
        "ktf,kdf->td", grad_all, gate_up_weight, preferred_element_type=F32
    ).astype(BF16)
    low_down_part = dot(hidden_all, down_input_factor, 1, 0)
    back_low_part = [dot(grad_all[k], gate_up_output_factor[k], 1, 1) for k in range(2)]
    small_part = pad(jnp.concatenate([*back_low_part, low_down_part], axis=1)).astype(BF16)

    part_width = small_part.shape[1]
    out_sum, in_sum, small_sum = communicate(
        lambda *refs: final_kernel(n_dp, tok_rows, *refs),
        "final_sums",
        [
            shape((tok_rows, width), F32),
            shape((tok_rows, width), F32),
            shape((total, part_width), F32),
        ],
        [
            pltpu.VMEM((n_dp - 1, tok_rows, width), BF16),
            pltpu.VMEM((n_dp - 1, tok_rows, width), BF16),
            pltpu.VMEM((n_dp - 1, total, part_width), BF16),
            *[dma((3, n_dp - 1))] * 2,
        ],
        2,
        (out_part, in_part, small_part),
    )

    low_all = small_all[:, : 2 * rank].reshape(total, 2, rank)
    upper_gradient = gradient_scale * jnp.stack(
        [dot(low_all[:, k], grad_all[k], 0, 0) for k in range(2)]
    )
    down_input_gradient = gradient_scale * dot(hidden_all, back_down, 0, 0)

    back_low = small_sum[:, : 2 * rank].astype(BF16)
    low_down = small_sum[:, 2 * rank : 3 * rank]
    down_output_gradient = gradient_scale * dot(low_down, cot.astype(F32), 0, 0, HIGHEST)
    lower_gradient = gradient_scale * jnp.stack(
        [dot(tok, back_low[:, k * rank : (k + 1) * rank], 0, 0) for k in range(2)]
    )
    dp_start = lax.axis_index("dp") * tok_rows
    back_low_rows = lax.dynamic_slice_in_dim(back_low, dp_start, tok_rows, 0)
    low_down_rows = lax.dynamic_slice_in_dim(low_down, dp_start, tok_rows, 0)
    output = out_sum + adapter_scale * dot(
        low_down_rows, down_output_factor.astype(F32), 1, 0, HIGHEST
    )
    input_grad = in_sum
    for k in range(2):
        input_grad = input_grad + adapter_scale * dot(
            back_low_rows[:, k * rank : (k + 1) * rank], gate_up_input_factor[k], 1, 1
        )
    return (
        output.astype(BF16),
        input_grad.astype(BF16),
        lower_gradient,
        upper_gradient,
        down_input_gradient,
        down_output_gradient,
    )


def solution(mesh):
    placed = (
        P("dp", "mp"),
        P(None, "mp", "dp"),
        P("dp", "mp"),
        P(None, "mp", None),
        P(None, None, "dp"),
        P("dp", None),
        P(None, "mp"),
        P("dp", "mp"),
    )
    return jax.shard_map(
        per_device,
        mesh=mesh,
        in_specs=placed,
        out_specs=(
            P("dp", "mp"),
            P("dp", "mp"),
            P(None, "mp", None),
            P(None, None, "dp"),
            P("dp", None),
            P(None, "mp"),
        ),
        check_vma=False,
    )
```

```python
import jax
import jax.numpy as jnp
from jax import lax
from jax.experimental import pallas as pl
from jax.experimental.pallas import tpu as pltpu
from jax.sharding import PartitionSpec as P

adapter_scale = 2.0
MESH = pl.DeviceIdType.MESH
F32 = jnp.float32
BF16 = jnp.bfloat16
HIGHEST = lax.Precision.HIGHEST


def dot(left, right, left_dim, right_dim, precision=None):
    return lax.dot_general(
        left,
        right,
        (((left_dim,), (right_dim,)), ((), ())),
        preferred_element_type=F32,
        precision=precision,
    )


def remote(axis, peer, source, target, send_sem, recv_sem):
    copy = pltpu.make_async_remote_copy(
        src_ref=source,
        dst_ref=target,
        send_sem=send_sem,
        recv_sem=recv_sem,
        device_id={axis: peer},
        device_id_type=MESH,
    )
    copy.start()
    return copy


def tile_of(size):
    return max(t for t in range(128, 1281, 128) if size % t == 0)


def layer_kernel(
    n_dp,
    n_outer,
    n_inner,
    rank,
    tok_ref,
    cot_ref,
    lower_ref,
    upper_ref,
    down_in_ref,
    down_out_ref,
    weight_hbm,
    down_hbm,
    tok_out,
    cot_out,
    small_out,
    hidden_out,
    grad_out,
    out_sum,
    in_sum,
    low_sum,
    weight,
    down,
    small_part,
    gate_part,
    up_part,
    back_part,
    wide_in,
    wide_sum,
    wide_far,
    small_in,
    small_mid,
    small_far,
    total_acc,
    out_part,
    in_part,
    low_part,
    out_far,
    in_far,
    low_far,
    load_sem,
    first_send,
    first_recv,
    inner_send,
    inner_recv,
    outer_send,
    outer_recv,
    gather_send,
    gather_recv,
    spread_send,
    spread_recv,
    last_send,
    last_recv,
):
    me_dp = lax.axis_index("dp")
    me = lax.axis_index("mp")
    outer = me // n_inner
    inner = lax.rem(me, n_inner)
    tok_rows = tok_ref.shape[0]
    total = tok_out.shape[0]
    rows = total // (n_outer * n_inner)
    hidden_size = down.shape[0]
    tile = tile_of(hidden_size)
    tiles = hidden_size // tile

    loads = [
        pltpu.make_async_copy(weight_hbm.at[0], weight.at[0], load_sem.at[0]),
        pltpu.make_async_copy(weight_hbm.at[1], weight.at[1], load_sem.at[1]),
        pltpu.make_async_copy(down_hbm, down, load_sem.at[2]),
    ]
    for load in loads:
        load.start()

    def place(o, i):
        return lax.rem(outer + o, n_outer) * n_inner + lax.rem(inner + i, n_inner)

    def block(index, size=rows):
        return pl.ds(pl.multiple_of(index * size, size), size)

    dp_peers = [lax.rem(me_dp + o, n_dp) for o in range(1, n_dp)]
    mp_peers = [place(0, i) for i in range(1, n_inner)] + [place(o, 0) for o in range(1, n_outer)]
    barrier = pltpu.get_barrier_semaphore()
    for axis, peers in (("dp", dp_peers), ("mp", mp_peers)):
        for peer in peers:
            pl.semaphore_signal(barrier, inc=1, device_id={axis: peer}, device_id_type=MESH)
    pl.semaphore_wait(barrier, len(dp_peers) + len(mp_peers))

    mine = block(me_dp, tok_rows)
    sent = []
    first = []
    for a, (source, target) in enumerate(((tok_ref, tok_out), (cot_ref, cot_out))):
        for o, peer in enumerate(dp_peers):
            first.append(
                remote("dp", peer, source, target.at[mine], first_send.at[a, o], first_recv.at[a, o])
            )
    sent += first
    tok_out[mine, :] = tok_ref[...]
    cot_out[mine, :] = cot_ref[...]

    order = sorted(range(1, n_outer), key=lambda o: -min(o, n_outer - o)) + [0]
    sources = (small_part, gate_part, up_part, back_part)

    def landing(a, *index):
        return small_in.at[index] if a == 0 else wide_in.at[(a - 1, *index)]

    def middle(a, o):
        return small_mid.at[o] if a == 0 else wide_sum.at[a - 1, o]

    def distant(a, o):
        return small_far.at[o] if a == 0 else wide_far.at[a - 1, o]

    near = {}

    def send_near(a):
        for o in order:
            for i in range(1, n_inner):
                near[a, o, i] = remote(
                    "mp",
                    place(0, i),
                    sources[a].at[block(place(o, i))],
                    landing(a, i - 1, o),
                    inner_send.at[a, i - 1, o],
                    inner_recv.at[a, i - 1, o],
                )
                sent.append(near[a, o, i])

    def columns(t):
        return pl.ds(pl.multiple_of(t * tile, tile), tile)

    for copy in first[: n_dp - 1]:
        copy.wait_recv()
    loads[0].wait()

    @pl.loop(0, tiles)
    def _(t):
        gate_part[:, columns(t)] = dot(tok_out[...], weight[0, :, columns(t)], 1, 0).astype(BF16)

    send_near(1)
    loads[1].wait()

    @pl.loop(0, tiles)
    def _(t):
        up_part[:, columns(t)] = dot(tok_out[...], weight[1, :, columns(t)], 1, 0).astype(BF16)

    for copy in first[n_dp - 1 :]:
        copy.wait_recv()
    pieces = [dot(tok_out[...], lower_ref[k], 1, 0) for k in range(2)]
    pieces.append(dot(cot_out[...], down_out_ref[...], 1, 1))
    pieces.append(jnp.zeros_like(pieces[0]))
    small_part[...] = jnp.concatenate(pieces, axis=1).astype(BF16)
    send_near(0)
    send_near(2)
    loads[2].wait()

    @pl.loop(0, tiles)
    def _(t):
        back_part[:, columns(t)] = dot(cot_out[...], down[columns(t), :], 1, 1).astype(BF16)

    send_near(3)
    far = {}

    def near_total(a, o):
        summed = sources[a][block(place(o, 0)), :].astype(F32)
        for i in range(1, n_inner):
            near[a, o, i].wait_recv()
            summed = summed + landing(a, i - 1, o)[...].astype(F32)
        return summed

    for a in (1, 0, 2, 3):
        for o in order[:-1]:
            middle(a, o - 1)[...] = near_total(a, o).astype(BF16)
            far[a, o] = remote(
                "mp",
                place(o, 0),
                middle(a, o - 1),
                distant(a, o - 1),
                outer_send.at[a, o - 1],
                outer_recv.at[a, o - 1],
            )
            sent.append(far[a, o])

    def full_total(a):
        summed = near_total(a, 0)
        for o in order[:-1]:
            far[a, o].wait_recv()
            summed = summed + distant(a, o - 1)[...].astype(F32)
        return summed

    arrived = {}
    spreads = {}
    outs = (small_out, hidden_out, grad_out.at[0], grad_out.at[1])

    def spread_block(a, o, source):
        for i in range(1, n_inner):
            spreads[a, o, i] = remote(
                "mp",
                place(0, i),
                source,
                source,
                spread_send.at[a, i - 1, o],
                spread_recv.at[a, i - 1, o],
            )
            sent.append(spreads[a, o, i])

    def give(a):
        source = outs[a].at[block(me)]
        for o in order[:-1]:
            arrived[a, o] = remote(
                "mp", place(o, 0), source, source, gather_send.at[a, o - 1], gather_recv.at[a, o - 1]
            )
            sent.append(arrived[a, o])
        spread_block(a, 0, source)

    def spread(a):
        for o in order[:-1]:
            arrived[a, o].wait_recv()
            spread_block(a, o, outs[a].at[block(place(n_outer - o, 0))])

    def complete(a):
        for o in order:
            for i in range(1, n_inner):
                spreads[a, o, i].wait_recv()

    gate = full_total(1)
    small = full_total(0)
    small_out[block(me), :] = small.astype(BF16)
    give(0)
    gate = gate + adapter_scale * dot(small[:, :rank], upper_ref[0].astype(F32), 1, 0, HIGHEST)
    sigma = 1.0 / (1.0 + jnp.exp(-gate))
    upper = full_total(2) + adapter_scale * dot(
        small[:, rank : 2 * rank], upper_ref[1].astype(F32), 1, 0, HIGHEST
    )
    hidden_out[block(me), :] = (gate * sigma * upper).astype(BF16)
    give(1)
    back_down = small[:, 2 * rank : 3 * rank].astype(BF16)
    back_adapter = adapter_scale * dot(back_down, down_in_ref[...], 1, 1)
    hidden_back = full_total(3) + back_adapter
    grad_out[0, block(me), :] = (
        hidden_back * upper * sigma * (1.0 + gate * (1.0 - sigma))
    ).astype(BF16)
    give(2)
    grad_out[1, block(me), :] = (hidden_back * gate * sigma).astype(BF16)
    give(3)
    spread(0)
    spread(1)
    spread(2)

    last = []

    def send_last(a, source, landing_ref):
        for o, peer in enumerate(dp_peers):
            cut = source if a == 0 else source.at[block(peer, tok_rows)]
            last.append(
                remote("dp", peer, cut, landing_ref.at[o], last_send.at[a, o], last_recv.at[a, o])
            )

    complete(0)
    complete(1)
    total_acc[...] = jnp.zeros_like(total_acc)

    @pl.loop(0, tiles)
    def _(t):
        total_acc[...] += dot(hidden_out[:, columns(t)], down[columns(t), :], 1, 0)

    out_part[...] = total_acc[...].astype(BF16)
    send_last(1, out_part, out_far)
    low_down = dot(hidden_out[...], down_in_ref[...], 1, 0)
    total_acc[...] = jnp.zeros_like(total_acc)
    spread(3)
    back_lows = []
    for k in range(2):
        complete(2 + k)

        @pl.loop(0, tiles)
        def _(t):
            total_acc[...] += dot(grad_out[k, :, columns(t)], weight[k, :, columns(t)], 1, 1)

        back_lows.append(dot(grad_out[k], upper_ref[k], 1, 1))
    low_part[...] = jnp.concatenate(
        [*back_lows, low_down, jnp.zeros_like(low_down)], axis=1
    ).astype(BF16)
    in_part[...] = total_acc[...].astype(BF16)
    send_last(0, low_part, low_far)
    send_last(2, in_part, in_far)

    for copy in last:
        copy.wait_recv()
    low_total = low_part[...].astype(F32)
    total_out = out_part[mine, :].astype(F32)
    total_in = in_part[mine, :].astype(F32)
    for o in range(n_dp - 1):
        low_total = low_total + low_far[o].astype(F32)
        total_out = total_out + out_far[o].astype(F32)
        total_in = total_in + in_far[o].astype(F32)
    low_sum[...] = low_total
    out_sum[...] = total_out
    in_sum[...] = total_in
    for copy in sent + last:
        copy.wait_send()


def shape(dims, dtype):
    return jax.ShapeDtypeStruct(dims, dtype)


def inner_size(n):
    size = 1
    while size * size * 4 <= n:
        size *= 2
    return size


def per_device(
    tokens,
    gate_up_weight,
    down_weight,
    gate_up_input_factor,
    gate_up_output_factor,
    down_input_factor,
    down_output_factor,
    cotangent,
):
    n_dp, n_mp = lax.axis_size("dp"), lax.axis_size("mp")
    tok_rows, width = tokens.shape
    rank, hidden = gate_up_output_factor.shape[1:]
    total = tok_rows * n_dp
    mp_rows = total // n_mp
    gradient_scale = adapter_scale * total ** (-0.5)
    dma = pltpu.SemaphoreType.DMA

    n_inner = inner_size(n_mp)
    n_outer = n_mp // n_inner
    small_width = 4 * rank
    vmem = pl.BlockSpec(memory_space=pltpu.VMEM)
    hbm = pl.BlockSpec(memory_space=pltpu.HBM)

    def buffer(*dims, dtype=BF16):
        return pltpu.VMEM(dims, dtype)

    tok, cot, small_all, hidden_all, grad_all, out_sum, in_sum, small_sum = pl.pallas_call(
        lambda *refs: layer_kernel(n_dp, n_outer, n_inner, rank, *refs),
        name="layer",
        out_shape=[
            shape((total, width), BF16),
            shape((total, width), BF16),
            shape((total, small_width), BF16),
            shape((total, hidden), BF16),
            shape((2, total, hidden), BF16),
            shape((tok_rows, width), F32),
            shape((tok_rows, width), F32),
            shape((total, small_width), F32),
        ],
        in_specs=[vmem] * 6 + [hbm] * 2,
        out_specs=[vmem] * 8,
        scratch_shapes=[
            buffer(2, width, hidden),
            buffer(hidden, width),
            buffer(total, small_width),
            buffer(total, hidden),
            buffer(total, hidden),
            buffer(total, hidden),
            buffer(3, n_inner - 1, n_outer, mp_rows, hidden),
            buffer(3, n_outer - 1, mp_rows, hidden),
            buffer(3, n_outer - 1, mp_rows, hidden),
            buffer(n_inner - 1, n_outer, mp_rows, small_width),
            buffer(n_outer - 1, mp_rows, small_width),
            buffer(n_outer - 1, mp_rows, small_width),
            buffer(total, width, dtype=F32),
            buffer(total, width),
            buffer(total, width),
            buffer(total, small_width),
            buffer(n_dp - 1, tok_rows, width),
            buffer(n_dp - 1, tok_rows, width),
            buffer(n_dp - 1, total, small_width),
            dma((3,)),
            *[dma((2, n_dp - 1))] * 2,
            *[dma((4, n_inner - 1, n_outer))] * 2,
            *[dma((4, n_outer - 1))] * 2,
            *[dma((4, n_outer - 1))] * 2,
            *[dma((4, n_inner - 1, n_outer))] * 2,
            *[dma((3, n_dp - 1))] * 2,
        ],
        compiler_params=pltpu.CompilerParams(
            collective_id=0, has_side_effects=True, vmem_limit_bytes=56 * 1024 * 1024
        ),
    )(
        tokens,
        cotangent,
        gate_up_input_factor,
        gate_up_output_factor,
        down_input_factor,
        down_output_factor,
        gate_up_weight,
        down_weight,
    )
    back_down = small_all[:, 2 * rank : 3 * rank]

    low_all = small_all[:, : 2 * rank].reshape(total, 2, rank)
    upper_gradient = gradient_scale * jnp.stack(
        [dot(low_all[:, k], grad_all[k], 0, 0) for k in range(2)]
    )
    down_input_gradient = gradient_scale * dot(hidden_all, back_down, 0, 0)

    back_low = small_sum[:, : 2 * rank].astype(BF16)
    low_down = small_sum[:, 2 * rank : 3 * rank]
    down_output_gradient = gradient_scale * dot(low_down, cot.astype(F32), 0, 0, HIGHEST)
    lower_gradient = gradient_scale * jnp.stack(
        [dot(tok, back_low[:, k * rank : (k + 1) * rank], 0, 0) for k in range(2)]
    )
    dp_start = lax.axis_index("dp") * tok_rows
    back_low_rows = lax.dynamic_slice_in_dim(back_low, dp_start, tok_rows, 0)
    low_down_rows = lax.dynamic_slice_in_dim(low_down, dp_start, tok_rows, 0)
    output = out_sum + adapter_scale * dot(
        low_down_rows, down_output_factor.astype(F32), 1, 0, HIGHEST
    )
    input_grad = in_sum
    for k in range(2):
        input_grad = input_grad + adapter_scale * dot(
            back_low_rows[:, k * rank : (k + 1) * rank], gate_up_input_factor[k], 1, 1
        )
    return (
        output.astype(BF16),
        input_grad.astype(BF16),
        lower_gradient,
        upper_gradient,
        down_input_gradient,
        down_output_gradient,
    )


def solution(mesh):
    placed = (
        P("dp", "mp"),
        P(None, "mp", "dp"),
        P("dp", "mp"),
        P(None, "mp", None),
        P(None, None, "dp"),
        P("dp", None),
        P(None, "mp"),
        P("dp", "mp"),
    )
    return jax.shard_map(
        per_device,
        mesh=mesh,
        in_specs=placed,
        out_specs=(
            P("dp", "mp"),
            P("dp", "mp"),
            P(None, "mp", None),
            P(None, None, "dp"),
            P("dp", None),
            P(None, "mp"),
        ),
        check_vma=False,
    )
```
